32 devices in a mesh: wl: 8 (over y, x, core), tile: 4 (over z).
Axes of the slice: x: 2, y: 2, z: 4, core: 2. Of those that a mesh axis runs over, the one named last changes fastest.
Arguments:
- forward: float32 [32, 2, 1024, 1024], P(('wl', 'tile')), may hold values from -6 to 6
- adjoint: float32 [32, 2, 1024, 1024], P(('wl', 'tile')), may hold values from -6 to 6
- mode: float32 [2, 1024], replicated, may hold values from -6 to 6
- target: float32 [32], P(('wl', 'tile')), may hold values from 0 to 2
- wl_index: int32 [32], P(('wl', 'tile')), may hold values from 0 to 31, each once
- tile_of: int32 [32], replicated, may hold values from 0 to 31, each once
- density: float32 [1024, 1024], P(('wl', 'tile')), may hold values from 0 to 1
Outputs:
- gradient: float32 [1024, 1024], P(('wl', 'tile'))
The draws below stay inside these ranges and needn't reach their ends.
All inputs are finite; a program needn't handle non-finite values.
Results may differ from the reference program's by a relative error of at most 0.00002.
Values sent between devices are 32-bit elements; how exact they have to be, the bound alone decides.
A program may use at most 64 MiB of HBM per device.

```python
import jax
import jax.numpy as jnp
from jax import lax

ROWS = 1024
COLS = 1024
NWL = 32
N_WL = 8
N_TILE = 4
DEVICES = 32


def block_scale(key, shape, cuts, least, high):
    def one(dim, shards_of):
        steps = jax.random.uniform(jax.random.fold_in(jax.random.fold_in(key, 6), dim), (shards_of,), jnp.float32, least / len(cuts), high / len(cuts))
        return jnp.repeat(jnp.exp(steps), shape[dim] // shards_of).reshape((-1,) + (1,) * (len(shape) - dim - 1))

    loudness = one(*cuts[0])
    for cut in cuts[1:]:
        loudness = loudness * one(*cut)
    return loudness


def bell_draw(own_key, dims, spread, most, shards=(), kind=jnp.bfloat16):
    loudness = block_scale(own_key, dims, shards, -0.22, 0.18) if shards else 1.0
    result = jax.random.normal(own_key, dims, jnp.float32) * spread * loudness
    return jnp.minimum(jnp.maximum(result, -most), most).astype(kind)


def setup_inputs(seed: int = 0) -> dict:
    key_list = jax.random.split(jax.random.key(seed), 8)
    return {
        "forward": bell_draw(key_list[0], (NWL, 2, ROWS, COLS), 1.0, 6.0, ((0, 32),), jnp.float32),
        "adjoint": bell_draw(key_list[1], (NWL, 2, ROWS, COLS), 1.0, 6.0, ((0, 32),), jnp.float32),
        "mode": bell_draw(key_list[2], (2, COLS), 1.0, 6.0, (), jnp.float32),
        "target": jnp.clip(2.0 * jax.random.uniform(key_list[3], (NWL,), jnp.float32) ** block_scale(key_list[3], (NWL,), ((0, 32),), -0.2, 0.2), 0.0, 2.0),
        "wl_index": jax.random.permutation(key_list[4], NWL).astype(jnp.int32),
        "tile_of": jax.random.permutation(key_list[5], DEVICES).astype(jnp.int32),
        "density": jnp.clip(1.0 * jax.random.uniform(key_list[6], (ROWS, COLS), jnp.float32) ** block_scale(key_list[6], (ROWS, COLS), ((0, 32),), -0.2, 0.2), 0.0, 1.0),
    }


def reference(forward, adjoint, mode, target, wl_index, tile_of, density):
    devices = N_WL * N_TILE
    mon = ROWS // 2
    line = forward[:, :, mon, :]
    over_re = lax.optimization_barrier(jnp.sum(line[:, 0] * mode[0] - line[:, 1] * mode[1], axis=1))
    over_im = lax.optimization_barrier(jnp.sum(line[:, 0] * mode[1] + line[:, 1] * mode[0], axis=1))
    fom = (over_re * over_re + over_im * over_im) / COLS
    scale = jnp.sum(fom) / NWL + 1.0
    weight = target - fom / scale
    freq = 1.0 + wl_index.astype(jnp.float32) / NWL

    def accumulate(total, items):
        fwd, adj, wgt, frq = items
        field = frq * frq * (fwd[0] * adj[0] - fwd[1] * adj[1])
        return (total + wgt * field, None)
    start = jnp.zeros((ROWS, COLS), jnp.float32)
    total, _ = lax.scan(accumulate, start, (forward, adjoint, weight, freq))
    tile_rows = ROWS // devices
    arranged = total.reshape(devices, tile_rows, COLS)[tile_of].reshape(ROWS, COLS)
    slope = 4.0 * (1.0 - jnp.tanh(4.0 * (density - 0.5)) ** 2)
    shaped = arranged * slope
    return shaped / jnp.sqrt(jnp.mean(shaped * shaped) + 1e-06)
```

```python
import functools

import jax
import jax.numpy as jnp
from jax import lax
from jax.experimental import pallas as pl
from jax.experimental.pallas import tpu as pltpu
from jax.sharding import PartitionSpec as P

MESH = pl.DeviceIdType.MESH
SUB = 8
LANES = 128
PIECES = 16
PATTERNS = ("AzBw", "BzAw")
SPACE = 0.3
LAG = 4.0
EARLY = 16
ORDER = ()


def plane(wide):
    cores = 2 if wide % 2 == 0 else 1
    chips = wide // cores
    first = max(f for f in range(1, chips + 1) if chips % f == 0 and f * f <= chips)
    return first, chips // first, cores


def digits_of(axis, size):
    out, stride, f = [], 1, 2
    while stride < size:
        while (size // stride) % f:
            f += 1
        out.append((axis, f, stride))
        stride *= f
    return out


def radix(step):
    n = 1
    for d in step:
        n *= d[1]
    return n


def steps_of(pattern, dims):
    parts = {"A": dims[0], "B": dims[1], "Z": dims[2], "z": dims[2][:1], "w": dims[2][1:]}
    return [tuple(parts[c]) for c in pattern if parts[c]]


def schedule(orders):
    ops = []
    if sorted(ORDER) == [(i, s) for i, steps in enumerate(orders) for s in range(-1, len(steps))]:
        return ORDER
    for i, steps in enumerate(orders):
        ops.append((i * SPACE, i, -1))
        for s in range(len(steps)):
            ops.append((i * SPACE + (s + 1) * LAG, i, s))
    return [(i, s) for _, i, s in sorted(ops)]


def kernel(
    sizes, orders, target, wl_index, tiles_in, mode_in, density_in, fwd, adj, shaped_out, norm_out,
    tile_of, mode, density, line, f_src, f_recv, w_src, w_recv, q_src, q_recv, slope, own, away, r0, recv,
    in_sem, side_sem, pair_sem, swap_sem, step_sem, *bufs,
):
    g1, g2, cores, deep, groups, parts, rows, cols = sizes
    devices = g1 * g2 * cores * deep
    tile_rows = rows // devices
    per_core = g1 * g2 * deep
    width = cols // parts
    pieces = groups * parts
    f_bufs, a_bufs = bufs[:groups], bufs[groups:]
    w_me, z_me = lax.axis_index("wl"), lax.axis_index("tile")
    c_me = w_me % cores
    me = (w_me // (cores * g2), (w_me // cores) % g2, z_me, c_me)
    dims = [digits_of(0, g1), digits_of(1, g2), digits_of(2, deep), digits_of(3, cores)]

    def shift(coords, digit, o):
        axis, f, stride = digit
        d = (coords[axis] // stride) % f
        moved = coords[axis] + ((d + o) % f - d) * stride
        return coords[:axis] + (moved,) + coords[axis + 1 :]

    def split(digits, index):
        out = []
        for d in digits:
            out.append(index % d[1])
            index = index // d[1]
        return out

    def at(coords):
        a, b, z, c = coords
        return ((a * g2 + b) * cores + c, z)

    def flat(coords):
        w, z = at(coords)
        return w * deep + z

    def move(digits, index):
        coords = me
        for d, o in zip(digits, split(digits, index)):
            if not isinstance(o, int) or o:
                coords = shift(coords, d, o)
        return coords

    every = [d for axis in dims for d in axis]
    far = lambda j: -sum(d[2] * (d[0] != 3) + 0.5 for d, o in zip(every, split(every, j)) if o)
    others = sorted(range(1, devices), key=far)
    other = {j: at(move(every, j)) for j in others}

    barrier = pltpu.get_barrier_semaphore()
    for j in others:
        pl.semaphore_signal(barrier, inc=1, device_id=other[j], device_id_type=MESH)

    mon = rows // 2
    mt, mk, ms = mon // tile_rows, (mon % tile_rows) // SUB, mon % SUB
    line_copy = pltpu.make_async_copy(fwd.at[:, mt, mk], line, in_sem.at[2 * groups])
    mode_copy = pltpu.make_async_copy(mode_in, mode, side_sem.at[0])
    tile_copy = pltpu.make_async_copy(tiles_in, tile_of, side_sem.at[1])
    density_copy = pltpu.make_async_copy(density_in, density, side_sem.at[2])
    for copy in (line_copy, mode_copy, tile_copy):
        copy.start()
    loads = []
    for k in range(groups):
        pair = (
            pltpu.make_async_copy(fwd.at[:, :, k], f_bufs[k], in_sem.at[2 * k]),
            pltpu.make_async_copy(adj.at[:, :, k], a_bufs[k], in_sem.at[2 * k + 1]),
        )
        loads.append(pair)
    for copy in loads[0]:
        copy.start()

    line_copy.wait()
    mode_copy.wait()
    for pair in loads[1:]:
        for copy in pair:
            copy.start()
    density_copy.start()
    re, im = line[0, ms : ms + 1, :], line[1, ms : ms + 1, :]
    m_re, m_im = mode[0:1, :], mode[1:2, :]
    over_re = jnp.sum(re * m_re - im * m_im, axis=1, keepdims=True)
    over_im = jnp.sum(re * m_im + im * m_re, axis=1, keepdims=True)
    fom = jnp.broadcast_to((over_re * over_re + over_im * over_im) / cols, (1, LANES))
    f_src[...] = fom
    freq = 1.0 + wl_index[0].astype(jnp.float32) / devices
    aim, part = target[0] * (freq * freq), fom * (freq * freq)
    w_src[0:1, :] = jnp.full((1, LANES), aim)
    w_src[1:2, :] = part

    pl.semaphore_wait(barrier, devices - 1)

    def share(src, dst, sems):
        for j in others:
            pltpu.make_async_remote_copy(
                src_ref=src, dst_ref=dst.at[j - 1], send_sem=side_sem.at[sems], recv_sem=side_sem.at[sems + 1],
                device_id=other[j], device_id_type=MESH,
            ).start()
        return pltpu.make_async_remote_copy(
            src_ref=dst, dst_ref=dst, send_sem=side_sem.at[sems], recv_sem=side_sem.at[sems + 1],
            device_id=other[others[0]], device_id_type=MESH,
        )

    f_copy = share(f_src, f_recv, 3)
    partner = at(move(dims[3], 1)) if cores > 1 else None

    def swap_of(src, dst, ssem, rsem):
        return pltpu.make_async_remote_copy(
            src_ref=src, dst_ref=dst, send_sem=ssem, recv_sem=rsem, device_id=partner, device_id_type=MESH
        )

    if cores > 1:
        w_copy = swap_of(w_src, w_recv, pair_sem.at[0], pair_sem.at[1])
        w_copy.start()

    flat_dims = dims[0] + dims[1] + dims[2]
    weights = []
    for steps in orders:
        weight, span = {}, per_core
        for step in steps:
            span //= radix(step)
            unit = span
            for d in step:
                weight[d] = unit
                unit *= d[1]
        weights.append(weight)
    kinds = sorted({tuple(w[d] for d in flat_dims) for w in weights})
    kind_of = [kinds.index(tuple(w[d] for d in flat_dims)) for w in weights]
    wide_dims = dims[0] + dims[1]

    tile_copy.wait()

    def build(k):
        for copy in loads[k]:
            copy.wait()
        for half in range(cores):

            @pl.loop(0, g1 * g2)
            def _(i):
                offs = split(wide_dims, i)
                coords = me
                for d, o in zip(wide_dims, offs):
                    coords = shift(coords, d, o)
                if half:
                    coords = shift(coords, dims[3][0], half)
                base = [sum(o * kind[n] for n, o in enumerate(offs)) for kind in kinds]
                for oz in range(deep):
                    zo = split(dims[2], oz)
                    there = coords
                    for d, o in zip(dims[2], zo):
                        if o:
                            there = shift(there, d, o)
                    t = tile_of[flat(there)]
                    for p in range(parts):
                        cs = slice(p * width, (p + 1) * width)
                        piece = k * parts + p
                        kind = kind_of[piece]
                        slot = base[kind] + sum(o * kinds[kind][len(wide_dims) + n] for n, o in enumerate(zo))
                        (away if half else own)[piece, slot] = (
                            f_bufs[k][0, t, :, cs] * a_bufs[k][0, t, :, cs]
                            - f_bufs[k][1, t, :, cs] * a_bufs[k][1, t, :, cs]
                        )

    def swap(piece):
        return swap_of(away.at[piece], r0.at[piece], pair_sem.at[2], swap_sem.at[piece])

    for k in range(groups):
        build(k)
        for piece in range(k * parts, (k + 1) * parts):
            if cores > 1 and piece < EARLY:
                swap(piece).start()

    density_copy.wait()
    slope[...] = 4.0 * (1.0 - jnp.tanh(4.0 * (density[...] - 0.5)) ** 2)

    f_copy.wait_recv()
    for piece in range(EARLY, pieces):
        if cores > 1:
            swap(piece).start()
    total_fom = fom + jnp.sum(f_recv[...], axis=0)
    scale = total_fom / devices + 1.0

    def wide_factor(a, b):
        return jnp.broadcast_to(jnp.concatenate([a - b / scale] * (width // LANES), axis=1), (SUB, width))

    factor = wide_factor(aim, part)
    if cores > 1:
        w_copy.wait_recv()
        other_factor = wide_factor(w_recv[0:1, :], w_recv[1:2, :])

    spans, bases = [], []
    for steps in orders:
        span, base, ss, bs = per_core, 0, [], []
        for step in steps:
            span //= radix(step)
            ss.append(span)
            bs.append(base)
            base += (radix(step) - 1) * span
        spans.append(ss)
        bases.append(bs)

    def start(piece, s):
        step, span, base = orders[piece][s], spans[piece][s], bases[piece][s]
        for j in range(1, radix(step)):
            pltpu.make_async_remote_copy(
                src_ref=own.at[piece, pl.ds(j * span, span)],
                dst_ref=recv.at[piece, pl.ds(base + (j - 1) * span, span)],
                send_sem=pair_sem.at[3], recv_sem=step_sem.at[piece, s],
                device_id=at(move(step, j)), device_id_type=MESH,
            ).start()

    def take(piece, s):
        step, span, base = orders[piece][s], spans[piece][s], bases[piece][s]
        got = recv.at[piece, pl.ds(base, (radix(step) - 1) * span)]
        pltpu.make_async_remote_copy(
            src_ref=got, dst_ref=got, send_sem=pair_sem.at[3], recv_sem=step_sem.at[piece, s],
            device_id=at(move(step, 1)), device_id_type=MESH,
        ).wait_recv()
        value = own[piece, :span]
        for j in range(radix(step) - 1):
            value = value + recv[piece, base + j * span : base + (j + 1) * span]
        return value

    squares = jnp.zeros((SUB, LANES), jnp.float32)
    for piece, s in schedule(orders):
        steps = orders[piece]
        if s < 0:
            if cores > 1:
                swap(piece).wait_recv()
                own[piece] = own[piece] * factor + r0[piece] * other_factor
            else:
                own[piece] = own[piece] * factor
            if steps:
                start(piece, 0)
        elif s < len(steps) - 1:
            own[piece, : spans[piece][s]] = take(piece, s)
            start(piece, s + 1)
        if s == len(steps) - 1:
            value = take(piece, s)[0] if steps else own[piece, 0]
            k, p = piece // parts, piece % parts
            rs, cs = slice(k * SUB, (k + 1) * SUB), slice(p * width, (p + 1) * width)
            shaped = value * slope[rs, cs]
            shaped_out[rs, cs] = shaped
            shaped = shaped * shaped
            for n in range(width // LANES):
                squares = squares + shaped[:, n * LANES : (n + 1) * LANES]
    mine = jnp.sum(squares, axis=0, keepdims=True)
    q_src[...] = mine
    q_copy = share(q_src, q_recv, 5)

    if cores > 1:
        w_copy.wait_send()
        swap_of(away, r0, pair_sem.at[2], pair_sem.at[2]).wait_send()
    if per_core > 1:
        sent = own.at[:, pl.ds(0, per_core - 1)]
        pltpu.make_async_remote_copy(
            src_ref=sent, dst_ref=sent, send_sem=pair_sem.at[3], recv_sem=pair_sem.at[3],
            device_id=other[others[0]], device_id_type=MESH,
        ).wait_send()
    f_copy.wait_send()
    q_copy.wait_recv()
    squares = jnp.sum(mine + jnp.sum(q_recv[...], axis=0), axis=1, keepdims=True)
    norm_out[...] = jnp.broadcast_to(jnp.sqrt(squares / (rows * cols) + 1e-06), (1, LANES))
    q_copy.wait_send()


def per_device(forward, adjoint, mode, target, wl_index, tile_of, density):
    wide, deep = lax.axis_size("wl"), lax.axis_size("tile")
    devices = wide * deep
    rows, cols = forward.shape[2:]
    g1, g2, cores = plane(wide)
    tile_rows = rows // devices
    groups = tile_rows // SUB
    parts = max(1, min(PIECES // groups, cols // LANES))
    pieces = groups * parts
    width = cols // parts
    per_core = g1 * g2 * deep
    dims = [digits_of(0, g1), digits_of(1, g2), digits_of(2, deep)]
    orders = [steps_of(PATTERNS[i % len(PATTERNS)], dims) for i in range(pieces)]
    fwd = forward.reshape(2, devices, groups, SUB, cols)
    adj = adjoint.reshape(2, devices, groups, SUB, cols)
    f32 = jnp.float32
    dma = pltpu.SemaphoreType.DMA
    block = lambda n: pltpu.VMEM((pieces, n, SUB, width), f32)
    sizes = (g1, g2, cores, deep, groups, parts, rows, cols)
    peers = max(devices - 1, 1)
    vmem = pl.BlockSpec(memory_space=pltpu.VMEM)
    smem = pl.BlockSpec(memory_space=pltpu.SMEM)
    hbm = pl.BlockSpec(memory_space=pl.ANY)
    shaped, norm = pl.pallas_call(
        functools.partial(kernel, sizes, orders),
        out_shape=(pltpu.VMEM((tile_rows, cols), f32), pltpu.VMEM((1, LANES), f32)),
        in_specs=[smem, smem, hbm, hbm, hbm, hbm, hbm],
        out_specs=(vmem, vmem),
        scratch_shapes=[
            pltpu.SMEM((devices,), jnp.int32),
            pltpu.VMEM(mode.shape, f32),
            pltpu.VMEM((tile_rows, cols), f32),
            pltpu.VMEM((2, SUB, cols), f32),
            pltpu.VMEM((1, LANES), f32),
            pltpu.VMEM((peers, 1, LANES), f32),
            pltpu.VMEM((2, LANES), f32),
            pltpu.VMEM((2, LANES), f32),
            pltpu.VMEM((1, LANES), f32),
            pltpu.VMEM((peers, 1, LANES), f32),
            pltpu.VMEM((tile_rows, cols), f32),
            block(per_core),
            block(per_core),
            block(per_core),
            block(per_core),
            dma((2 * groups + 1,)),
            dma((7,)),
            dma((4,)),
            dma((pieces,)),
            dma((pieces, max(len(o) for o in orders))),
        ]
        + [pltpu.VMEM((2, devices, SUB, cols), f32)] * (2 * groups),
        compiler_params=pltpu.CompilerParams(
            collective_id=0, has_side_effects=True, vmem_limit_bytes=60 * 2**20
        ),
        name="assemble",
    )(target, wl_index, tile_of, mode, density, fwd, adj)
    return shaped / norm[0, 0]


def solution(mesh):
    in_specs = (
        P(("wl", "tile"), None, None, None),
        P(("wl", "tile"), None, None, None),
        P(),
        P(("wl", "tile")),
        P(("wl", "tile")),
        P(),
        P(("wl", "tile"), None),
    )
    out_specs = P(("wl", "tile"), None)
    return jax.shard_map(
        per_device, mesh=mesh, in_specs=in_specs, out_specs=out_specs, check_vma=False
    )
```

```python
import functools

import jax
import jax.numpy as jnp
from jax import lax
from jax.experimental import pallas as pl
from jax.experimental.pallas import tpu as pltpu
from jax.sharding import PartitionSpec as P

MESH = pl.DeviceIdType.MESH
SUB = 8
LANES = 128
PIECES = 16
PATTERNS = ('B.z.w.A', 'A.B.zw', 'w.A.z.B', 'B.w.A.z', 'A.z.B.w', 'A.B.w.z', 'A.w.z.B', 'A.B.zw', 'z.A.B.w', 'B.A.z.w', 'B.z.A.w', 'z.B.A.w', 'B.w.A.z', 'w.A.B.z', 'A.B.zw', 'B.A.zw')
SPACE = 0.3
LAG = 4.0
EARLY = 16
PRE = 0
DELAY = 2000
FIRST = 1
ORDER = ((0, -1), (1, -1), (2, -1), (3, -1), (4, -1), (5, -1), (6, -1), (7, -1), (8, -1), (9, -1), (10, -1), (11, -1), (12, -1), (13, -1), (14, -1), (15, -1), (0, 0), (1, 0), (2, 0), (3, 0), (4, 0), (5, 0), (6, 0), (7, 0), (8, 0), (9, 0), (10, 0), (11, 0), (12, 0), (13, 0), (14, 0), (15, 0), (0, 1), (1, 1), (2, 1), (3, 1), (4, 1), (5, 1), (6, 1), (7, 1), (8, 1), (9, 1), (10, 1), (11, 1), (12, 1), (13, 1), (14, 1), (15, 1), (0, 2), (1, 2), (2, 2), (3, 2), (4, 2), (5, 2), (6, 2), (8, 2), (9, 2), (10, 2), (11, 2), (12, 2), (13, 2), (0, 3), (2, 3), (3, 3), (4, 3), (12, 3), (13, 3), (6, 3), (8, 3), (7, 2), (9, 3), (5, 3), (14, 2), (15, 2), (10, 3), (11, 3))


def plane(wide):
    cores = 2 if wide % 2 == 0 else 1
    chips = wide // cores
    first = max(f for f in range(1, chips + 1) if chips % f == 0 and f * f <= chips)
    return first, chips // first, cores


def digits_of(axis, size):
    out, stride, f = [], 1, 2
    while stride < size:
        while (size // stride) % f:
            f += 1
        out.append((axis, f, stride))
        stride *= f
    return out


def radix(step):
    n = 1
    for d in step:
        n *= d[1]
    return n


def steps_of(pattern, dims):
    parts = {"A": dims[0], "B": dims[1], "z": dims[2][:1], "w": dims[2][1:]}
    steps = [tuple(d for c in step for d in parts[c]) for step in pattern.split(".")]
    return [step for step in steps if step]


def schedule(orders):
    ops = []
    if sorted(ORDER) == [(i, s) for i, steps in enumerate(orders) for s in range(-1, len(steps))]:
        return ORDER
    for i, steps in enumerate(orders):
        ops.append((i * SPACE, i, -1))
        for s in range(len(steps)):
            ops.append((i * SPACE + (s + 1) * LAG, i, s))
    return [(i, s) for _, i, s in sorted(ops)]


def kernel(
    sizes, orders, target, wl_index, tiles_in, mode_in, density_in, fwd, adj, shaped_out, norm_out,
    tile_of, mode, density, line, f_src, f_recv, w_src, w_recv, q_src, q_recv, slope, own, away, r0, recv,
    in_sem, side_sem, pair_sem, swap_sem, step_sem, *bufs,
):
    g1, g2, cores, deep, groups, parts, rows, cols = sizes
    devices = g1 * g2 * cores * deep
    tile_rows = rows // devices
    per_core = g1 * g2 * deep
    width = cols // parts
    pieces = groups * parts
    f_bufs, a_bufs = bufs[:groups], bufs[groups:]
    w_me, z_me = lax.axis_index("wl"), lax.axis_index("tile")
    c_me = w_me % cores
    me = (w_me // (cores * g2), (w_me // cores) % g2, z_me, c_me)
    dims = [digits_of(0, g1), digits_of(1, g2), digits_of(2, deep), digits_of(3, cores)]

    def shift(coords, digit, o):
        axis, f, stride = digit
        d = (coords[axis] // stride) % f
        moved = coords[axis] + ((d + o) % f - d) * stride
        return coords[:axis] + (moved,) + coords[axis + 1 :]

    def split(digits, index):
        out = []
        for d in digits:
            out.append(index % d[1])
            index = index // d[1]
        return out

    def at(coords):
        a, b, z, c = coords
        return ((a * g2 + b) * cores + c, z)

    def flat(coords):
        w, z = at(coords)
        return w * deep + z

    def move(digits, index):
        coords = me
        for d, o in zip(digits, split(digits, index)):
            if not isinstance(o, int) or o:
                coords = shift(coords, d, o)
        return coords

    every = [d for axis in dims for d in axis]
    far = lambda j: -sum(d[2] * (d[0] != 3) + 0.5 for d, o in zip(every, split(every, j)) if o)
    others = sorted(range(1, devices), key=far)
    other = {j: at(move(every, j)) for j in others}

    barrier = pltpu.get_barrier_semaphore()
    for j in others:
        pl.semaphore_signal(barrier, inc=1, device_id=other[j], device_id_type=MESH)

    mon = rows // 2
    mt, mk, ms = mon // tile_rows, (mon % tile_rows) // SUB, mon % SUB
    line_copy = pltpu.make_async_copy(fwd.at[:, mt, mk], line, in_sem.at[2 * groups])
    mode_copy = pltpu.make_async_copy(mode_in, mode, side_sem.at[0])
    tile_copy = pltpu.make_async_copy(tiles_in, tile_of, side_sem.at[1])
    density_copy = pltpu.make_async_copy(density_in, density, side_sem.at[2])
    for copy in (line_copy, mode_copy, tile_copy):
        copy.start()
    loads = []
    for k in range(groups):
        pair = (
            pltpu.make_async_copy(fwd.at[:, :, k], f_bufs[k], in_sem.at[2 * k]),
            pltpu.make_async_copy(adj.at[:, :, k], a_bufs[k], in_sem.at[2 * k + 1]),
        )
        loads.append(pair)
    for pair in loads[:FIRST]:
        for copy in pair:
            copy.start()

    line_copy.wait()
    mode_copy.wait()
    for pair in loads[FIRST:]:
        for copy in pair:
            copy.start()
    density_copy.start()
    re, im = line[0, ms : ms + 1, :], line[1, ms : ms + 1, :]
    m_re, m_im = mode[0:1, :], mode[1:2, :]
    over_re = jnp.sum(re * m_re - im * m_im, axis=1, keepdims=True)
    over_im = jnp.sum(re * m_im + im * m_re, axis=1, keepdims=True)
    fom = jnp.broadcast_to((over_re * over_re + over_im * over_im) / cols, (1, LANES))
    f_src[...] = fom
    freq = 1.0 + wl_index[0].astype(jnp.float32) / devices
    aim, part = target[0] * (freq * freq), fom * (freq * freq)
    w_src[0:1, :] = jnp.full((1, LANES), aim)
    w_src[1:2, :] = part

    flat_dims = dims[0] + dims[1] + dims[2]
    weights = []
    for steps in orders:
        weight, span = {}, per_core
        for step in steps:
            span //= radix(step)
            unit = span
            for d in step:
                weight[d] = unit
                unit *= d[1]
        weights.append(weight)
    kinds = sorted({tuple(w[d] for d in flat_dims) for w in weights})
    kind_of = [kinds.index(tuple(w[d] for d in flat_dims)) for w in weights]
    wide_dims = dims[0] + dims[1]

    tile_copy.wait()

    def build(k):
        for copy in loads[k]:
            copy.wait()
        for half in range(cores):

            @pl.loop(0, g1 * g2)
            def _(i):
                offs = split(wide_dims, i)
                coords = me
                for d, o in zip(wide_dims, offs):
                    coords = shift(coords, d, o)
                if half:
                    coords = shift(coords, dims[3][0], half)
                base = [sum(o * kind[n] for n, o in enumerate(offs)) for kind in kinds]
                for oz in range(deep):
                    zo = split(dims[2], oz)
                    there = coords
                    for d, o in zip(dims[2], zo):
                        if o:
                            there = shift(there, d, o)
                    t = tile_of[flat(there)]
                    for p in range(parts):
                        cs = slice(p * width, (p + 1) * width)
                        piece = k * parts + p
                        kind = kind_of[piece]
                        slot = base[kind] + sum(o * kinds[kind][len(wide_dims) + n] for n, o in enumerate(zo))
                        (away if half else own)[piece, slot] = (
                            f_bufs[k][0, t, :, cs] * a_bufs[k][0, t, :, cs]
                            - f_bufs[k][1, t, :, cs] * a_bufs[k][1, t, :, cs]
                        )

    for k in range(min(PRE, groups)):
        build(k)

    pl.semaphore_wait(barrier, devices - 1)

    def share(src, dst, sems):
        for j in others:
            pltpu.make_async_remote_copy(
                src_ref=src, dst_ref=dst.at[j - 1], send_sem=side_sem.at[sems], recv_sem=side_sem.at[sems + 1],
                device_id=other[j], device_id_type=MESH,
            ).start()
        return pltpu.make_async_remote_copy(
            src_ref=dst, dst_ref=dst, send_sem=side_sem.at[sems], recv_sem=side_sem.at[sems + 1],
            device_id=other[others[0]], device_id_type=MESH,
        )

    f_copy = share(f_src, f_recv, 3)
    partner = at(move(dims[3], 1)) if cores > 1 else None

    def swap_of(src, dst, ssem, rsem):
        return pltpu.make_async_remote_copy(
            src_ref=src, dst_ref=dst, send_sem=ssem, recv_sem=rsem, device_id=partner, device_id_type=MESH
        )

    if cores > 1:
        w_copy = swap_of(w_src, w_recv, pair_sem.at[0], pair_sem.at[1])
        w_copy.start()

    def swap(piece):
        return swap_of(away.at[piece], r0.at[piece], pair_sem.at[2], swap_sem.at[piece])

    for k in range(groups):
        if k >= PRE:
            build(k)
        for piece in range(k * parts, (k + 1) * parts):
            if cores > 1 and piece < EARLY:
                swap(piece).start()

    density_copy.wait()
    slope[...] = 4.0 * (1.0 - jnp.tanh(4.0 * (density[...] - 0.5)) ** 2)

    f_copy.wait_recv()
    for piece in range(EARLY, pieces):
        if cores > 1:
            swap(piece).start()
    total_fom = fom + jnp.sum(f_recv[...], axis=0)
    scale = total_fom / devices + 1.0

    def wide_factor(a, b):
        return jnp.broadcast_to(jnp.concatenate([a - b / scale] * (width // LANES), axis=1), (SUB, width))

    factor = wide_factor(aim, part)
    if cores > 1:
        w_copy.wait_recv()
        other_factor = wide_factor(w_recv[0:1, :], w_recv[1:2, :])

    spans, bases = [], []
    for steps in orders:
        span, base, ss, bs = per_core, 0, [], []
        for step in steps:
            span //= radix(step)
            ss.append(span)
            bs.append(base)
            base += (radix(step) - 1) * span
        spans.append(ss)
        bases.append(bs)

    def start(piece, s):
        step, span, base = orders[piece][s], spans[piece][s], bases[piece][s]
        for j in range(1, radix(step)):
            pltpu.make_async_remote_copy(
                src_ref=own.at[piece, pl.ds(j * span, span)],
                dst_ref=recv.at[piece, pl.ds(base + (j - 1) * span, span)],
                send_sem=pair_sem.at[3], recv_sem=step_sem.at[piece, s],
                device_id=at(move(step, j)), device_id_type=MESH,
            ).start()

    def take(piece, s):
        step, span, base = orders[piece][s], spans[piece][s], bases[piece][s]
        got = recv.at[piece, pl.ds(base, (radix(step) - 1) * span)]
        pltpu.make_async_remote_copy(
            src_ref=got, dst_ref=got, send_sem=pair_sem.at[3], recv_sem=step_sem.at[piece, s],
            device_id=at(move(step, 1)), device_id_type=MESH,
        ).wait_recv()
        value = own[piece, :span]
        for j in range(radix(step) - 1):
            value = value + recv[piece, base + j * span : base + (j + 1) * span]
        return value

    if DELAY:
        @pl.when(c_me == 1)
        def _():
            pl.delay(DELAY)

    squares = jnp.zeros((SUB, LANES), jnp.float32)
    for piece, s in schedule(orders):
        steps = orders[piece]
        if s < 0:
            if cores > 1:
                swap(piece).wait_recv()
                own[piece] = own[piece] * factor + r0[piece] * other_factor
            else:
                own[piece] = own[piece] * factor
            if steps:
                start(piece, 0)
        elif s < len(steps) - 1:
            own[piece, : spans[piece][s]] = take(piece, s)
            start(piece, s + 1)
        if s == len(steps) - 1:
            value = take(piece, s)[0] if steps else own[piece, 0]
            k, p = piece // parts, piece % parts
            rs, cs = slice(k * SUB, (k + 1) * SUB), slice(p * width, (p + 1) * width)
            shaped = value * slope[rs, cs]
            shaped_out[rs, cs] = shaped
            shaped = shaped * shaped
            for n in range(width // LANES):
                squares = squares + shaped[:, n * LANES : (n + 1) * LANES]
    mine = jnp.sum(squares, axis=0, keepdims=True)
    q_src[...] = mine
    q_copy = share(q_src, q_recv, 5)

    if cores > 1:
        w_copy.wait_send()
        swap_of(away, r0, pair_sem.at[2], pair_sem.at[2]).wait_send()
    if per_core > 1:
        sent = own.at[:, pl.ds(0, per_core - 1)]
        pltpu.make_async_remote_copy(
            src_ref=sent, dst_ref=sent, send_sem=pair_sem.at[3], recv_sem=pair_sem.at[3],
            device_id=other[others[0]], device_id_type=MESH,
        ).wait_send()
    f_copy.wait_send()
    q_copy.wait_recv()
    squares = jnp.sum(mine + jnp.sum(q_recv[...], axis=0), axis=1, keepdims=True)
    norm_out[...] = jnp.broadcast_to(jnp.sqrt(squares / (rows * cols) + 1e-06), (1, LANES))
    q_copy.wait_send()


def per_device(forward, adjoint, mode, target, wl_index, tile_of, density):
    wide, deep = lax.axis_size("wl"), lax.axis_size("tile")
    devices = wide * deep
    rows, cols = forward.shape[2:]
    g1, g2, cores = plane(wide)
    tile_rows = rows // devices
    groups = tile_rows // SUB
    parts = max(1, min(PIECES // groups, cols // LANES))
    pieces = groups * parts
    width = cols // parts
    per_core = g1 * g2 * deep
    dims = [digits_of(0, g1), digits_of(1, g2), digits_of(2, deep)]
    orders = [steps_of(PATTERNS[i % len(PATTERNS)], dims) for i in range(pieces)]
    fwd = forward.reshape(2, devices, groups, SUB, cols)
    adj = adjoint.reshape(2, devices, groups, SUB, cols)
    f32 = jnp.float32
    dma = pltpu.SemaphoreType.DMA
    block = lambda n: pltpu.VMEM((pieces, n, SUB, width), f32)
    sizes = (g1, g2, cores, deep, groups, parts, rows, cols)
    peers = max(devices - 1, 1)
    vmem = pl.BlockSpec(memory_space=pltpu.VMEM)
    smem = pl.BlockSpec(memory_space=pltpu.SMEM)
    hbm = pl.BlockSpec(memory_space=pl.ANY)
    shaped, norm = pl.pallas_call(
        functools.partial(kernel, sizes, orders),
        out_shape=(pltpu.VMEM((tile_rows, cols), f32), pltpu.VMEM((1, LANES), f32)),
        in_specs=[smem, smem, hbm, hbm, hbm, hbm, hbm],
        out_specs=(vmem, vmem),
        scratch_shapes=[
            pltpu.SMEM((devices,), jnp.int32),
            pltpu.VMEM(mode.shape, f32),
            pltpu.VMEM((tile_rows, cols), f32),
            pltpu.VMEM((2, SUB, cols), f32),
            pltpu.VMEM((1, LANES), f32),
            pltpu.VMEM((peers, 1, LANES), f32),
            pltpu.VMEM((2, LANES), f32),
            pltpu.VMEM((2, LANES), f32),
            pltpu.VMEM((1, LANES), f32),
            pltpu.VMEM((peers, 1, LANES), f32),
            pltpu.VMEM((tile_rows, cols), f32),
            block(per_core),
            block(per_core),
            block(per_core),
            block(per_core),
            dma((2 * groups + 1,)),
            dma((7,)),
            dma((4,)),
            dma((pieces,)),
            dma((pieces, max(len(o) for o in orders))),
        ]
        + [pltpu.VMEM((2, devices, SUB, cols), f32)] * (2 * groups),
        compiler_params=pltpu.CompilerParams(
            collective_id=0, has_side_effects=True, vmem_limit_bytes=60 * 2**20
        ),
        name="assemble",
    )(target, wl_index, tile_of, mode, density, fwd, adj)
    return shaped / norm[0, 0]


def solution(mesh):
    in_specs = (
        P(("wl", "tile"), None, None, None),
        P(("wl", "tile"), None, None, None),
        P(),
        P(("wl", "tile")),
        P(("wl", "tile")),
        P(),
        P(("wl", "tile"), None),
    )
    out_specs = P(("wl", "tile"), None)
    return jax.shard_map(
        per_device, mesh=mesh, in_specs=in_specs, out_specs=out_specs, check_vma=False
    )
```

```python
import functools

import jax
import jax.numpy as jnp
from jax import lax
from jax.experimental import pallas as pl
from jax.experimental.pallas import tpu as pltpu
from jax.sharding import PartitionSpec as P

MESH = pl.DeviceIdType.MESH
SUB = 8
LANES = 128
PIECES = 16
PATTERNS = ('B.z.w.A', 'A.B.zw', 'w.A.z.B', 'B.w.A.z', 'A.z.B.w', 'A.B.w.z', 'A.w.z.B', 'A.B.zw', 'z.A.B.w', 'B.A.z.w', 'B.z.A.w', 'z.B.A.w', 'B.w.A.z', 'w.A.B.z', 'A.B.zw', 'B.A.zw')
SPACE = 0.3
LAG = 4.0
DELAY = 2000
EAGER = 2
ORDER = ((0, -1), (1, -1), (2, -1), (3, -1), (4, -1), (5, -1), (6, -1), (7, -1), (8, -1), (9, -1), (10, -1), (11, -1), (12, -1), (13, -1), (14, -1), (15, -1), (0, 0), (1, 0), (2, 0), (3, 0), (4, 0), (5, 0), (6, 0), (7, 0), (8, 0), (9, 0), (10, 0), (11, 0), (12, 0), (13, 0), (14, 0), (15, 0), (0, 1), (1, 1), (2, 1), (3, 1), (4, 1), (5, 1), (6, 1), (7, 1), (8, 1), (9, 1), (10, 1), (11, 1), (12, 1), (13, 1), (14, 1), (15, 1), (0, 2), (1, 2), (2, 2), (3, 2), (4, 2), (5, 2), (6, 2), (8, 2), (9, 2), (10, 2), (11, 2), (12, 2), (13, 2), (0, 3), (2, 3), (3, 3), (4, 3), (12, 3), (13, 3), (6, 3), (8, 3), (7, 2), (9, 3), (5, 3), (14, 2), (15, 2), (10, 3), (11, 3))


def plane(wide):
    cores = 2 if wide % 2 == 0 else 1
    chips = wide // cores
    first = max(f for f in range(1, chips + 1) if chips % f == 0 and f * f <= chips)
    return first, chips // first, cores


def digits_of(axis, size):
    out, stride, f = [], 1, 2
    while stride < size:
        while (size // stride) % f:
            f += 1
        out.append((axis, f, stride))
        stride *= f
    return out


def radix(step):
    n = 1
    for d in step:
        n *= d[1]
    return n


def steps_of(pattern, dims):
    parts = {"A": dims[0], "B": dims[1], "z": dims[2][:1], "w": dims[2][1:]}
    steps = [tuple(d for c in step for d in parts[c]) for step in pattern.split(".")]
    return [step for step in steps if step]


def schedule(orders):
    ops = []
    if sorted(ORDER) == [(i, s) for i, steps in enumerate(orders) for s in range(-1, len(steps))]:
        return ORDER
    for i, steps in enumerate(orders):
        ops.append((i * SPACE, i, -1))
        for s in range(len(steps)):
            ops.append((i * SPACE + (s + 1) * LAG, i, s))
    return [(i, s) for _, i, s in sorted(ops)]


def kernel(
    sizes, orders, target, wl_index, tiles_in, mode_in, density_in, fwd, adj, shaped_out, norm_out,
    tile_of, mode, density, line, f_src, f_recv, w_src, w_recv, q_src, q_recv, slope, own, away, r0, recv, raw,
    in_sem, side_sem, pair_sem, swap_sem, step_sem, *bufs,
):
    g1, g2, cores, deep, groups, parts, rows, cols = sizes
    devices = g1 * g2 * cores * deep
    tile_rows = rows // devices
    per_core = g1 * g2 * deep
    width = cols // parts
    pieces = groups * parts
    f_bufs, a_bufs = bufs[:groups], bufs[groups:]
    w_me, z_me = lax.axis_index("wl"), lax.axis_index("tile")
    c_me = w_me % cores
    me = (w_me // (cores * g2), (w_me // cores) % g2, z_me, c_me)
    dims = [digits_of(0, g1), digits_of(1, g2), digits_of(2, deep), digits_of(3, cores)]

    def shift(coords, digit, o):
        axis, f, stride = digit
        d = (coords[axis] // stride) % f
        moved = coords[axis] + ((d + o) % f - d) * stride
        return coords[:axis] + (moved,) + coords[axis + 1 :]

    def split(digits, index):
        out = []
        for d in digits:
            out.append(index % d[1])
            index = index // d[1]
        return out

    def at(coords):
        a, b, z, c = coords
        return ((a * g2 + b) * cores + c, z)

    def flat(coords):
        w, z = at(coords)
        return w * deep + z

    def move(digits, index):
        coords = me
        for d, o in zip(digits, split(digits, index)):
            if not isinstance(o, int) or o:
                coords = shift(coords, d, o)
        return coords

    every = [d for axis in dims for d in axis]
    far = lambda j: -sum(d[2] * (d[0] != 3) + 0.5 for d, o in zip(every, split(every, j)) if o)
    others = sorted(range(1, devices), key=far)
    other = {j: at(move(every, j)) for j in others}

    barrier = pltpu.get_barrier_semaphore()
    for j in others:
        pl.semaphore_signal(barrier, inc=1, device_id=other[j], device_id_type=MESH)

    mon = rows // 2
    mt, mk, ms = mon // tile_rows, (mon % tile_rows) // SUB, mon % SUB
    line_copy = pltpu.make_async_copy(fwd.at[:, mt, mk], line, in_sem.at[2 * groups])
    mode_copy = pltpu.make_async_copy(mode_in, mode, side_sem.at[0])
    tile_copy = pltpu.make_async_copy(tiles_in, tile_of, side_sem.at[1])
    density_copy = pltpu.make_async_copy(density_in, density, side_sem.at[2])
    for copy in (line_copy, mode_copy, tile_copy):
        copy.start()
    loads = []
    for k in range(groups):
        pair = (
            pltpu.make_async_copy(fwd.at[:, :, k], f_bufs[k], in_sem.at[2 * k]),
            pltpu.make_async_copy(adj.at[:, :, k], a_bufs[k], in_sem.at[2 * k + 1]),
        )
        loads.append(pair)
    for pair in loads[:1]:
        for copy in pair:
            copy.start()

    line_copy.wait()
    mode_copy.wait()
    for pair in loads[1:]:
        for copy in pair:
            copy.start()
    density_copy.start()
    re, im = line[0, ms : ms + 1, :], line[1, ms : ms + 1, :]
    m_re, m_im = mode[0:1, :], mode[1:2, :]
    over_re = jnp.sum(re * m_re - im * m_im, axis=1, keepdims=True)
    over_im = jnp.sum(re * m_im + im * m_re, axis=1, keepdims=True)
    fom = jnp.broadcast_to((over_re * over_re + over_im * over_im) / cols, (1, LANES))
    f_src[...] = fom
    freq = 1.0 + wl_index[0].astype(jnp.float32) / devices
    aim, part = target[0] * (freq * freq), fom * (freq * freq)
    w_src[0:1, :] = jnp.full((1, LANES), aim)
    w_src[1:2, :] = part

    flat_dims = dims[0] + dims[1] + dims[2]
    weights = []
    for steps in orders:
        weight, span = {}, per_core
        for step in steps:
            span //= radix(step)
            unit = span
            for d in step:
                weight[d] = unit
                unit *= d[1]
        weights.append(weight)
    kinds = sorted({tuple(w[d] for d in flat_dims) for w in weights})
    kind_of = [kinds.index(tuple(w[d] for d in flat_dims)) for w in weights]
    wide_dims = dims[0] + dims[1]

    tile_copy.wait()

    def build(k):
        for copy in loads[k]:
            copy.wait()
        for half in range(cores):

            @pl.loop(0, g1 * g2)
            def _(i):
                offs = split(wide_dims, i)
                coords = me
                for d, o in zip(wide_dims, offs):
                    coords = shift(coords, d, o)
                if half:
                    coords = shift(coords, dims[3][0], half)
                base = [sum(o * kind[n] for n, o in enumerate(offs)) for kind in kinds]
                for oz in range(deep):
                    zo = split(dims[2], oz)
                    there = coords
                    for d, o in zip(dims[2], zo):
                        if o:
                            there = shift(there, d, o)
                    t = tile_of[flat(there)]
                    for p in range(parts):
                        cs = slice(p * width, (p + 1) * width)
                        piece = k * parts + p
                        kind = kind_of[piece]
                        slot = base[kind] + sum(o * kinds[kind][len(wide_dims) + n] for n, o in enumerate(zo))
                        (away if half else own)[piece, slot] = (
                            f_bufs[k][0, t, :, cs] * a_bufs[k][0, t, :, cs]
                            - f_bufs[k][1, t, :, cs] * a_bufs[k][1, t, :, cs]
                        )

    pl.semaphore_wait(barrier, devices - 1)

    def share(src, dst, sems):
        for j in others:
            pltpu.make_async_remote_copy(
                src_ref=src, dst_ref=dst.at[j - 1], send_sem=side_sem.at[sems], recv_sem=side_sem.at[sems + 1],
                device_id=other[j], device_id_type=MESH,
            ).start()
        return pltpu.make_async_remote_copy(
            src_ref=dst, dst_ref=dst, send_sem=side_sem.at[sems], recv_sem=side_sem.at[sems + 1],
            device_id=other[others[0]], device_id_type=MESH,
        )

    f_copy = share(f_src, f_recv, 3)
    partner = at(move(dims[3], 1)) if cores > 1 else None
    eager = range(min(EAGER, parts)) if cores == 2 and per_core > 1 else range(0)
    links = [(e, j, h) for e in eager for h in range(2) for j in range(1, radix(orders[e][0]))]

    def across(e, j, h):
        return at(move(list(orders[e][0]) + dims[3] * h, j + h * radix(orders[e][0])))

    def swap_of(src, dst, ssem, rsem):
        return pltpu.make_async_remote_copy(
            src_ref=src, dst_ref=dst, send_sem=ssem, recv_sem=rsem, device_id=partner, device_id_type=MESH
        )

    if cores > 1:
        for n, where in enumerate([partner] + [across(*link) for link in links]):
            pltpu.make_async_remote_copy(
                src_ref=w_src, dst_ref=w_recv.at[n], send_sem=pair_sem.at[0], recv_sem=pair_sem.at[1],
                device_id=where, device_id_type=MESH,
            ).start()
        w_copy = swap_of(w_recv, w_recv, pair_sem.at[0], pair_sem.at[1])

    def kept(piece):
        return per_core // radix(orders[piece][0]) if piece in eager else per_core

    def swap(piece):
        part = pl.ds(0, kept(piece))
        return swap_of(away.at[piece, part], r0.at[piece, part], pair_sem.at[2], swap_sem.at[piece])

    def swapped(k):
        part = pl.ds(k * parts, parts)
        return swap_of(away.at[part], r0.at[part], pair_sem.at[2], swap_sem.at[parts - 1 + k])

    def group_swap(piece):
        return swap_of(away.at[piece], r0.at[piece], pair_sem.at[2], swap_sem.at[parts - 1 + piece // parts])

    def swap_out(piece):
        (swap(piece) if piece < parts else group_swap(piece)).start()

    def send_raw(e):
        step, span = orders[e][0], kept(e)
        for h, src in enumerate((own, away)):
            for j in range(1, radix(step)):
                pltpu.make_async_remote_copy(
                    src_ref=src.at[e, pl.ds(j * span, span)],
                    dst_ref=raw.at[e, h, pl.ds((j - 1) * span, span)],
                    send_sem=pair_sem.at[2 + (h == 0)], recv_sem=step_sem.at[e, 0],
                    device_id=across(e, j, h), device_id_type=MESH,
                ).start()

    for k in range(groups):
        build(k)
        for piece in range(k * parts, (k + 1) * parts):
            if piece in eager:
                send_raw(piece)
        for piece in range(k * parts, (k + 1) * parts):
            if cores > 1:
                swap_out(piece)

    density_copy.wait()
    slope[...] = 4.0 * (1.0 - jnp.tanh(4.0 * (density[...] - 0.5)) ** 2)

    f_copy.wait_recv()
    total_fom = fom + jnp.sum(f_recv[...], axis=0)
    scale = total_fom / devices + 1.0

    def wide_factor(a, b):
        return jnp.broadcast_to(jnp.concatenate([a - b / scale] * (width // LANES), axis=1), (SUB, width))

    factor = wide_factor(aim, part)
    if cores > 1:
        w_copy.wait_recv()
        other_factor, *link_factors = [
            wide_factor(w_recv[n, 0:1, :], w_recv[n, 1:2, :]) for n in range(1 + len(links))
        ]
        link_factor = dict(zip(links, link_factors))

    spans, bases = [], []
    for steps in orders:
        span, base, ss, bs = per_core, 0, [], []
        for step in steps:
            span //= radix(step)
            ss.append(span)
            bs.append(base)
            base += (radix(step) - 1) * span
        spans.append(ss)
        bases.append(bs)

    def start(piece, s):
        step, span, base = orders[piece][s], spans[piece][s], bases[piece][s]
        for j in range(1, radix(step)):
            pltpu.make_async_remote_copy(
                src_ref=own.at[piece, pl.ds(j * span, span)],
                dst_ref=recv.at[piece, pl.ds(base + (j - 1) * span, span)],
                send_sem=pair_sem.at[3], recv_sem=step_sem.at[piece, s],
                device_id=at(move(step, j)), device_id_type=MESH,
            ).start()

    def take(piece, s):
        step, span, base = orders[piece][s], spans[piece][s], bases[piece][s]
        if s == 0 and piece in eager:
            got = raw.at[piece, :, pl.ds(0, (radix(step) - 1) * span)]
            pltpu.make_async_remote_copy(
                src_ref=got, dst_ref=got, send_sem=pair_sem.at[3], recv_sem=step_sem.at[piece, 0],
                device_id=at(move(step, 1)), device_id_type=MESH,
            ).wait_recv()
            value = own[piece, :span]
            for h in range(2):
                for j in range(1, radix(step)):
                    value = value + raw[piece, h, (j - 1) * span : j * span] * link_factor[piece, j, h]
            return value
        got = recv.at[piece, pl.ds(base, (radix(step) - 1) * span)]
        pltpu.make_async_remote_copy(
            src_ref=got, dst_ref=got, send_sem=pair_sem.at[3], recv_sem=step_sem.at[piece, s],
            device_id=at(move(step, 1)), device_id_type=MESH,
        ).wait_recv()
        value = own[piece, :span]
        for j in range(radix(step) - 1):
            value = value + recv[piece, base + j * span : base + (j + 1) * span]
        return value

    if DELAY:
        @pl.when(c_me == 1)
        def _():
            pl.delay(DELAY)

    squares = jnp.zeros((SUB, LANES), jnp.float32)
    opened = set()
    for piece, s in schedule(orders):
        steps = orders[piece]
        if s < 0:
            if cores > 1:
                if piece < parts:
                    swap(piece).wait_recv()
                elif piece // parts not in opened:
                    opened.add(piece // parts)
                    swapped(piece // parts).wait_recv()
                part = slice(0, kept(piece))
                own[piece, part] = own[piece, part] * factor + r0[piece, part] * other_factor
            else:
                own[piece] = own[piece] * factor
            if steps and piece not in eager:
                start(piece, 0)
        elif s < len(steps) - 1:
            own[piece, : spans[piece][s]] = take(piece, s)
            start(piece, s + 1)
        if s == len(steps) - 1:
            value = take(piece, s)[0] if steps else own[piece, 0]
            k, p = piece // parts, piece % parts
            rs, cs = slice(k * SUB, (k + 1) * SUB), slice(p * width, (p + 1) * width)
            shaped = value * slope[rs, cs]
            shaped_out[rs, cs] = shaped
            shaped = shaped * shaped
            for n in range(width // LANES):
                squares = squares + shaped[:, n * LANES : (n + 1) * LANES]
    mine = jnp.sum(squares, axis=0, keepdims=True)
    q_src[...] = mine
    q_copy = share(q_src, q_recv, 5)

    if cores > 1:
        w_copy.wait_send()
        swap_of(away, r0, pair_sem.at[2], pair_sem.at[2]).wait_send()
    if per_core > 1:
        sent = own.at[:, pl.ds(0, per_core - 1)]
        pltpu.make_async_remote_copy(
            src_ref=sent, dst_ref=sent, send_sem=pair_sem.at[3], recv_sem=pair_sem.at[3],
            device_id=other[others[0]], device_id_type=MESH,
        ).wait_send()
    f_copy.wait_send()
    q_copy.wait_recv()
    squares = jnp.sum(mine + jnp.sum(q_recv[...], axis=0), axis=1, keepdims=True)
    norm_out[...] = jnp.broadcast_to(jnp.sqrt(squares / (rows * cols) + 1e-06), (1, LANES))
    q_copy.wait_send()


def per_device(forward, adjoint, mode, target, wl_index, tile_of, density):
    wide, deep = lax.axis_size("wl"), lax.axis_size("tile")
    devices = wide * deep
    rows, cols = forward.shape[2:]
    g1, g2, cores = plane(wide)
    tile_rows = rows // devices
    groups = tile_rows // SUB
    parts = max(1, min(PIECES // groups, cols // LANES))
    pieces = groups * parts
    width = cols // parts
    per_core = g1 * g2 * deep
    dims = [digits_of(0, g1), digits_of(1, g2), digits_of(2, deep)]
    orders = [steps_of(PATTERNS[i % len(PATTERNS)], dims) for i in range(pieces)]
    eager = orders[: min(EAGER, parts)] if cores == 2 and per_core > 1 else []
    messages = 1 + sum(2 * (radix(steps[0]) - 1) for steps in eager)
    fwd = forward.reshape(2, devices, groups, SUB, cols)
    adj = adjoint.reshape(2, devices, groups, SUB, cols)
    f32 = jnp.float32
    dma = pltpu.SemaphoreType.DMA
    block = lambda n: pltpu.VMEM((pieces, n, SUB, width), f32)
    sizes = (g1, g2, cores, deep, groups, parts, rows, cols)
    peers = max(devices - 1, 1)
    vmem = pl.BlockSpec(memory_space=pltpu.VMEM)
    smem = pl.BlockSpec(memory_space=pltpu.SMEM)
    hbm = pl.BlockSpec(memory_space=pl.ANY)
    shaped, norm = pl.pallas_call(
        functools.partial(kernel, sizes, orders),
        out_shape=(pltpu.VMEM((tile_rows, cols), f32), pltpu.VMEM((1, LANES), f32)),
        in_specs=[smem, smem, hbm, hbm, hbm, hbm, hbm],
        out_specs=(vmem, vmem),
        scratch_shapes=[
            pltpu.SMEM((devices,), jnp.int32),
            pltpu.VMEM(mode.shape, f32),
            pltpu.VMEM((tile_rows, cols), f32),
            pltpu.VMEM((2, SUB, cols), f32),
            pltpu.VMEM((1, LANES), f32),
            pltpu.VMEM((peers, 1, LANES), f32),
            pltpu.VMEM((2, LANES), f32),
            pltpu.VMEM((messages, 2, LANES), f32),
            pltpu.VMEM((1, LANES), f32),
            pltpu.VMEM((peers, 1, LANES), f32),
            pltpu.VMEM((tile_rows, cols), f32),
            block(per_core),
            block(per_core),
            block(per_core),
            block(per_core),
            pltpu.VMEM((max(EAGER, 1), 2, per_core, SUB, width), f32),
            dma((2 * groups + 1,)),
            dma((7,)),
            dma((4,)),
            dma((parts + groups - 1,)),
            dma((pieces, max(len(o) for o in orders))),
        ]
        + [pltpu.VMEM((2, devices, SUB, cols), f32)] * (2 * groups),
        compiler_params=pltpu.CompilerParams(
            collective_id=0, has_side_effects=True, vmem_limit_bytes=60 * 2**20
        ),
        name="assemble",
    )(target, wl_index, tile_of, mode, density, fwd, adj)
    return shaped / norm[0, 0]


def solution(mesh):
    in_specs = (
        P(("wl", "tile"), None, None, None),
        P(("wl", "tile"), None, None, None),
        P(),
        P(("wl", "tile")),
        P(("wl", "tile")),
        P(),
        P(("wl", "tile"), None),
    )
    out_specs = P(("wl", "tile"), None)
    return jax.shard_map(
        per_device, mesh=mesh, in_specs=in_specs, out_specs=out_specs, check_vma=False
    )
```

```python
import functools

import jax
import jax.numpy as jnp
from jax import lax
from jax.experimental import pallas as pl
from jax.experimental.pallas import tpu as pltpu
from jax.sharding import PartitionSpec as P

MESH = pl.DeviceIdType.MESH
SUB = 8
LANES = 128
PIECES = 16
PATTERNS = ('Az.B.w', 'B.w.A.z', 'z.B.A.w', 'B.A.z.w', 'A.w.B.z', 'A.w.B.z', 'B.A.zw', 'B.A.zw', 'z.B.A.w', 'A.Bz.w', 'B.w.Az', 'B.A.zw', 'A.B.zw', 'A.Bz.w', 'w.A.Bz', 'z.AB.w')
SPACE = 0.3
LAG = 4.0
DELAY = 2800
EAGER = 2
ORDER = ((0, -1), (1, -1), (2, -1), (3, -1), (4, -1), (5, -1), (6, -1), (7, -1), (8, -1), (9, -1), (10, -1), (11, -1), (12, -1), (13, -1), (14, -1), (15, -1), (0, 0), (1, 0), (2, 0), (3, 0), (4, 0), (5, 0), (6, 0), (7, 0), (8, 0), (9, 0), (10, 0), (11, 0), (12, 0), (13, 0), (14, 0), (15, 0), (0, 1), (1, 1), (2, 1), (3, 1), (4, 1), (5, 1), (6, 1), (7, 1), (8, 1), (9, 1), (10, 1), (11, 1), (12, 1), (13, 1), (14, 1), (15, 1), (1, 2), (2, 2), (3, 2), (4, 2), (5, 2), (8, 2), (9, 2), (10, 2), (14, 2), (15, 2), (1, 3), (4, 3), (11, 2), (7, 2), (0, 2), (5, 3), (6, 2), (12, 2), (13, 2), (3, 3), (2, 3), (8, 3))


def plane(wide):
    cores = 2 if wide % 2 == 0 else 1
    chips = wide // cores
    first = max(f for f in range(1, chips + 1) if chips % f == 0 and f * f <= chips)
    return first, chips // first, cores


def digits_of(axis, size):
    out, stride, f = [], 1, 2
    while stride < size:
        while (size // stride) % f:
            f += 1
        out.append((axis, f, stride))
        stride *= f
    return out


def radix(step):
    n = 1
    for d in step:
        n *= d[1]
    return n


def steps_of(pattern, dims):
    parts = {"A": dims[0], "B": dims[1], "z": dims[2][:1], "w": dims[2][1:]}
    steps = [tuple(d for c in step for d in parts[c]) for step in pattern.split(".")]
    return [step for step in steps if step]


def schedule(orders):
    ops = []
    if sorted(ORDER) == [(i, s) for i, steps in enumerate(orders) for s in range(-1, len(steps))]:
        return ORDER
    for i, steps in enumerate(orders):
        ops.append((i * SPACE, i, -1))
        for s in range(len(steps)):
            ops.append((i * SPACE + (s + 1) * LAG, i, s))
    return [(i, s) for _, i, s in sorted(ops)]


def kernel(
    sizes, orders, target, wl_index, tiles_in, mode_in, density_in, fwd, adj, shaped_out, norm_out,
    tile_of, mode, density, line, f_src, f_recv, w_src, w_recv, q_src, q_recv, slope, own, away, r0, recv, raw,
    in_sem, side_sem, pair_sem, swap_sem, step_sem, *bufs,
):
    g1, g2, cores, deep, groups, parts, rows, cols = sizes
    devices = g1 * g2 * cores * deep
    tile_rows = rows // devices
    per_core = g1 * g2 * deep
    width = cols // parts
    pieces = groups * parts
    f_bufs, a_bufs = bufs[:groups], bufs[groups:]
    w_me, z_me = lax.axis_index("wl"), lax.axis_index("tile")
    c_me = w_me % cores
    me = (w_me // (cores * g2), (w_me // cores) % g2, z_me, c_me)
    dims = [digits_of(0, g1), digits_of(1, g2), digits_of(2, deep), digits_of(3, cores)]

    def shift(coords, digit, o):
        axis, f, stride = digit
        d = (coords[axis] // stride) % f
        moved = coords[axis] + ((d + o) % f - d) * stride
        return coords[:axis] + (moved,) + coords[axis + 1 :]

    def split(digits, index):
        out = []
        for d in digits:
            out.append(index % d[1])
            index = index // d[1]
        return out

    def at(coords):
        a, b, z, c = coords
        return ((a * g2 + b) * cores + c, z)

    def flat(coords):
        w, z = at(coords)
        return w * deep + z

    def move(digits, index):
        coords = me
        for d, o in zip(digits, split(digits, index)):
            if not isinstance(o, int) or o:
                coords = shift(coords, d, o)
        return coords

    every = [d for axis in dims for d in axis]
    far = lambda j: -sum(d[2] * (d[0] != 3) + 0.5 for d, o in zip(every, split(every, j)) if o)
    others = sorted(range(1, devices), key=far)
    other = {j: at(move(every, j)) for j in others}

    barrier = pltpu.get_barrier_semaphore()
    for j in others:
        pl.semaphore_signal(barrier, inc=1, device_id=other[j], device_id_type=MESH)

    mon = rows // 2
    mt, mk, ms = mon // tile_rows, (mon % tile_rows) // SUB, mon % SUB
    line_copy = pltpu.make_async_copy(fwd.at[:, mt, mk], line, in_sem.at[2 * groups])
    mode_copy = pltpu.make_async_copy(mode_in, mode, side_sem.at[0])
    tile_copy = pltpu.make_async_copy(tiles_in, tile_of, side_sem.at[1])
    density_copy = pltpu.make_async_copy(density_in, density, side_sem.at[2])
    for copy in (line_copy, mode_copy, tile_copy):
        copy.start()
    loads = []
    for k in range(groups):
        pair = (
            pltpu.make_async_copy(fwd.at[:, :, k], f_bufs[k], in_sem.at[2 * k]),
            pltpu.make_async_copy(adj.at[:, :, k], a_bufs[k], in_sem.at[2 * k + 1]),
        )
        loads.append(pair)
    for pair in loads[:1]:
        for copy in pair:
            copy.start()

    line_copy.wait()
    mode_copy.wait()
    for pair in loads[1:]:
        for copy in pair:
            copy.start()
    density_copy.start()
    re, im = line[0, ms : ms + 1, :], line[1, ms : ms + 1, :]
    m_re, m_im = mode[0:1, :], mode[1:2, :]
    over_re = jnp.sum(re * m_re - im * m_im, axis=1, keepdims=True)
    over_im = jnp.sum(re * m_im + im * m_re, axis=1, keepdims=True)
    fom = jnp.broadcast_to((over_re * over_re + over_im * over_im) / cols, (1, LANES))
    f_src[...] = fom
    freq = 1.0 + wl_index[0].astype(jnp.float32) / devices
    aim, part = target[0] * (freq * freq), fom * (freq * freq)
    w_src[0:1, :] = jnp.full((1, LANES), aim)
    w_src[1:2, :] = part

    sem_of = {}
    for piece, steps in enumerate(orders):
        for s in range(len(steps)):
            sem_of[piece, s] = len(sem_of)
    flat_dims = dims[0] + dims[1] + dims[2]
    weights = []
    for steps in orders:
        weight, span = {}, per_core
        for step in steps:
            span //= radix(step)
            unit = span
            for d in step:
                weight[d] = unit
                unit *= d[1]
        weights.append(weight)
    kinds = sorted({tuple(w[d] for d in flat_dims) for w in weights})
    kind_of = [kinds.index(tuple(w[d] for d in flat_dims)) for w in weights]
    wide_dims = dims[0] + dims[1]

    tile_copy.wait()

    def build(k):
        for copy in loads[k]:
            copy.wait()
        for half in range(cores):

            @pl.loop(0, g1 * g2)
            def _(i):
                offs = split(wide_dims, i)
                coords = me
                for d, o in zip(wide_dims, offs):
                    coords = shift(coords, d, o)
                if half:
                    coords = shift(coords, dims[3][0], half)
                base = [sum(o * kind[n] for n, o in enumerate(offs)) for kind in kinds]
                for oz in range(deep):
                    zo = split(dims[2], oz)
                    there = coords
                    for d, o in zip(dims[2], zo):
                        if o:
                            there = shift(there, d, o)
                    t = tile_of[flat(there)]
                    for p in range(parts):
                        cs = slice(p * width, (p + 1) * width)
                        piece = k * parts + p
                        kind = kind_of[piece]
                        slot = base[kind] + sum(o * kinds[kind][len(wide_dims) + n] for n, o in enumerate(zo))
                        (away if half else own)[piece, slot] = (
                            f_bufs[k][0, t, :, cs] * a_bufs[k][0, t, :, cs]
                            - f_bufs[k][1, t, :, cs] * a_bufs[k][1, t, :, cs]
                        )

    pl.semaphore_wait(barrier, devices - 1)

    def share(src, dst, sems):
        for j in others:
            pltpu.make_async_remote_copy(
                src_ref=src, dst_ref=dst.at[j - 1], send_sem=side_sem.at[sems], recv_sem=side_sem.at[sems + 1],
                device_id=other[j], device_id_type=MESH,
            ).start()
        return pltpu.make_async_remote_copy(
            src_ref=dst, dst_ref=dst, send_sem=side_sem.at[sems], recv_sem=side_sem.at[sems + 1],
            device_id=other[others[0]], device_id_type=MESH,
        )

    f_copy = share(f_src, f_recv, 3)
    partner = at(move(dims[3], 1)) if cores > 1 else None
    eager = range(min(EAGER, parts)) if cores == 2 and per_core > 1 else range(0)
    links = [(e, j, h) for e in eager for h in range(2) for j in range(1, radix(orders[e][0]))]

    def across(e, j, h):
        return at(move(list(orders[e][0]) + dims[3] * h, j + h * radix(orders[e][0])))

    def swap_of(src, dst, ssem, rsem):
        return pltpu.make_async_remote_copy(
            src_ref=src, dst_ref=dst, send_sem=ssem, recv_sem=rsem, device_id=partner, device_id_type=MESH
        )

    if cores > 1:
        for n, where in enumerate([partner] + [across(*link) for link in links]):
            pltpu.make_async_remote_copy(
                src_ref=w_src, dst_ref=w_recv.at[n], send_sem=pair_sem.at[0], recv_sem=pair_sem.at[1],
                device_id=where, device_id_type=MESH,
            ).start()
        w_copy = swap_of(w_recv, w_recv, pair_sem.at[0], pair_sem.at[1])

    def kept(piece):
        return per_core // radix(orders[piece][0]) if piece in eager else per_core

    def swap(piece):
        part = pl.ds(0, kept(piece))
        return swap_of(away.at[piece, part], r0.at[piece, part], pair_sem.at[2], swap_sem.at[piece])

    def swapped(k):
        part = pl.ds(k * parts, parts)
        return swap_of(away.at[part], r0.at[part], pair_sem.at[2], swap_sem.at[parts - 1 + k])

    def group_swap(piece):
        return swap_of(away.at[piece], r0.at[piece], pair_sem.at[2], swap_sem.at[parts - 1 + piece // parts])

    def swap_out(piece):
        (swap(piece) if piece < parts else group_swap(piece)).start()

    def send_raw(e):
        step, span = orders[e][0], kept(e)
        for h, src in enumerate((own, away)):
            for j in range(1, radix(step)):
                pltpu.make_async_remote_copy(
                    src_ref=src.at[e, pl.ds(j * span, span)],
                    dst_ref=raw.at[e, h, pl.ds((j - 1) * span, span)],
                    send_sem=pair_sem.at[2 + (h == 0)], recv_sem=step_sem.at[sem_of[e, 0]],
                    device_id=across(e, j, h), device_id_type=MESH,
                ).start()

    for k in range(groups):
        build(k)
        for piece in range(k * parts, (k + 1) * parts):
            if piece in eager:
                send_raw(piece)
        for piece in range(k * parts, (k + 1) * parts):
            if cores > 1:
                swap_out(piece)

    density_copy.wait()
    slope[...] = 4.0 * (1.0 - jnp.tanh(4.0 * (density[...] - 0.5)) ** 2)

    f_copy.wait_recv()
    total_fom = fom + jnp.sum(f_recv[...], axis=0)
    scale = total_fom / devices + 1.0

    def wide_factor(a, b):
        return jnp.broadcast_to(jnp.concatenate([a - b / scale] * (width // LANES), axis=1), (SUB, width))

    factor = wide_factor(aim, part)
    if cores > 1:
        w_copy.wait_recv()
        other_factor, *link_factors = [
            wide_factor(w_recv[n, 0:1, :], w_recv[n, 1:2, :]) for n in range(1 + len(links))
        ]
        link_factor = dict(zip(links, link_factors))

    spans, bases = [], []
    for steps in orders:
        span, base, ss, bs = per_core, 0, [], []
        for step in steps:
            span //= radix(step)
            ss.append(span)
            bs.append(base)
            base += (radix(step) - 1) * span
        spans.append(ss)
        bases.append(bs)

    def start(piece, s):
        step, span, base = orders[piece][s], spans[piece][s], bases[piece][s]
        for j in range(1, radix(step)):
            pltpu.make_async_remote_copy(
                src_ref=own.at[piece, pl.ds(j * span, span)],
                dst_ref=recv.at[piece, pl.ds(base + (j - 1) * span, span)],
                send_sem=pair_sem.at[3], recv_sem=step_sem.at[sem_of[piece, s]],
                device_id=at(move(step, j)), device_id_type=MESH,
            ).start()

    def take(piece, s):
        step, span, base = orders[piece][s], spans[piece][s], bases[piece][s]
        if s == 0 and piece in eager:
            got = raw.at[piece, :, pl.ds(0, (radix(step) - 1) * span)]
            pltpu.make_async_remote_copy(
                src_ref=got, dst_ref=got, send_sem=pair_sem.at[3], recv_sem=step_sem.at[sem_of[piece, 0]],
                device_id=at(move(step, 1)), device_id_type=MESH,
            ).wait_recv()
            value = own[piece, :span]
            for h in range(2):
                for j in range(1, radix(step)):
                    value = value + raw[piece, h, (j - 1) * span : j * span] * link_factor[piece, j, h]
            return value
        got = recv.at[piece, pl.ds(base, (radix(step) - 1) * span)]
        pltpu.make_async_remote_copy(
            src_ref=got, dst_ref=got, send_sem=pair_sem.at[3], recv_sem=step_sem.at[sem_of[piece, s]],
            device_id=at(move(step, 1)), device_id_type=MESH,
        ).wait_recv()
        value = own[piece, :span]
        for j in range(radix(step) - 1):
            value = value + recv[piece, base + j * span : base + (j + 1) * span]
        return value

    if DELAY:
        @pl.when(c_me == 1)
        def _():
            pl.delay(DELAY)

    squares = jnp.zeros((SUB, LANES), jnp.float32)
    opened = set()
    for piece, s in schedule(orders):
        steps = orders[piece]
        if s < 0:
            if cores > 1:
                if piece < parts:
                    swap(piece).wait_recv()
                elif piece // parts not in opened:
                    opened.add(piece // parts)
                    swapped(piece // parts).wait_recv()
                part = slice(0, kept(piece))
                own[piece, part] = own[piece, part] * factor + r0[piece, part] * other_factor
            else:
                own[piece] = own[piece] * factor
            if steps and piece not in eager:
                start(piece, 0)
        elif s < len(steps) - 1:
            own[piece, : spans[piece][s]] = take(piece, s)
            start(piece, s + 1)
        if s == len(steps) - 1:
            value = take(piece, s)[0] if steps else own[piece, 0]
            k, p = piece // parts, piece % parts
            rs, cs = slice(k * SUB, (k + 1) * SUB), slice(p * width, (p + 1) * width)
            shaped = value * slope[rs, cs]
            shaped_out[rs, cs] = shaped
            shaped = shaped * shaped
            for n in range(width // LANES):
                squares = squares + shaped[:, n * LANES : (n + 1) * LANES]
    mine = jnp.sum(squares, axis=0, keepdims=True)
    q_src[...] = mine
    q_copy = share(q_src, q_recv, 5)

    if cores > 1:
        w_copy.wait_send()
        swap_of(away, r0, pair_sem.at[2], pair_sem.at[2]).wait_send()
    if per_core > 1:
        sent = own.at[:, pl.ds(0, per_core - 1)]
        pltpu.make_async_remote_copy(
            src_ref=sent, dst_ref=sent, send_sem=pair_sem.at[3], recv_sem=pair_sem.at[3],
            device_id=other[others[0]], device_id_type=MESH,
        ).wait_send()
    f_copy.wait_send()
    q_copy.wait_recv()
    squares = jnp.sum(mine + jnp.sum(q_recv[...], axis=0), axis=1, keepdims=True)
    norm_out[...] = jnp.broadcast_to(jnp.sqrt(squares / (rows * cols) + 1e-06), (1, LANES))
    q_copy.wait_send()


def per_device(forward, adjoint, mode, target, wl_index, tile_of, density):
    wide, deep = lax.axis_size("wl"), lax.axis_size("tile")
    devices = wide * deep
    rows, cols = forward.shape[2:]
    g1, g2, cores = plane(wide)
    tile_rows = rows // devices
    groups = tile_rows // SUB
    parts = max(1, min(PIECES // groups, cols // LANES))
    pieces = groups * parts
    width = cols // parts
    per_core = g1 * g2 * deep
    dims = [digits_of(0, g1), digits_of(1, g2), digits_of(2, deep)]
    orders = [steps_of(PATTERNS[i % len(PATTERNS)], dims) for i in range(pieces)]
    eager = orders[: min(EAGER, parts)] if cores == 2 and per_core > 1 else []
    messages = 1 + sum(2 * (radix(steps[0]) - 1) for steps in eager)
    fwd = forward.reshape(2, devices, groups, SUB, cols)
    adj = adjoint.reshape(2, devices, groups, SUB, cols)
    f32 = jnp.float32
    dma = pltpu.SemaphoreType.DMA
    block = lambda n: pltpu.VMEM((pieces, n, SUB, width), f32)
    sizes = (g1, g2, cores, deep, groups, parts, rows, cols)
    peers = max(devices - 1, 1)
    vmem = pl.BlockSpec(memory_space=pltpu.VMEM)
    smem = pl.BlockSpec(memory_space=pltpu.SMEM)
    hbm = pl.BlockSpec(memory_space=pl.ANY)
    shaped, norm = pl.pallas_call(
        functools.partial(kernel, sizes, orders),
        out_shape=(pltpu.VMEM((tile_rows, cols), f32), pltpu.VMEM((1, LANES), f32)),
        in_specs=[smem, smem, hbm, hbm, hbm, hbm, hbm],
        out_specs=(vmem, vmem),
        scratch_shapes=[
            pltpu.SMEM((devices,), jnp.int32),
            pltpu.VMEM(mode.shape, f32),
            pltpu.VMEM((tile_rows, cols), f32),
            pltpu.VMEM((2, SUB, cols), f32),
            pltpu.VMEM((1, LANES), f32),
            pltpu.VMEM((peers, 1, LANES), f32),
            pltpu.VMEM((2, LANES), f32),
            pltpu.VMEM((messages, 2, LANES), f32),
            pltpu.VMEM((1, LANES), f32),
            pltpu.VMEM((peers, 1, LANES), f32),
            pltpu.VMEM((tile_rows, cols), f32),
            block(per_core),
            block(per_core),
            block(per_core),
            block(per_core),
            pltpu.VMEM((max(EAGER, 1), 2, per_core, SUB, width), f32),
            dma((2 * groups + 1,)),
            dma((7,)),
            dma((4,)),
            dma((parts + groups - 1,)),
            dma((max(sum(len(steps) for steps in orders), 1),)),
        ]
        + [pltpu.VMEM((2, devices, SUB, cols), f32)] * (2 * groups),
        compiler_params=pltpu.CompilerParams(
            collective_id=0, has_side_effects=True, vmem_limit_bytes=60 * 2**20
        ),
        name="assemble",
    )(target, wl_index, tile_of, mode, density, fwd, adj)
    return shaped / norm[0, 0]


def solution(mesh):
    in_specs = (
        P(("wl", "tile"), None, None, None),
        P(("wl", "tile"), None, None, None),
        P(),
        P(("wl", "tile")),
        P(("wl", "tile")),
        P(),
        P(("wl", "tile"), None),
    )
    out_specs = P(("wl", "tile"), None)
    return jax.shard_map(
        per_device, mesh=mesh, in_specs=in_specs, out_specs=out_specs, check_vma=False
    )
```

```python
import functools

import jax
import jax.numpy as jnp
from jax import lax
from jax.experimental import pallas as pl
from jax.experimental.pallas import tpu as pltpu
from jax.sharding import PartitionSpec as P

MESH = pl.DeviceIdType.MESH
SUB = 8
LANES = 128
PIECES = 16
PATTERNS = ('Az.B.w', 'B.w.A.z', 'z.B.A.w', 'B.A.z.w', 'A.w.B.z', 'A.w.B.z', 'B.A.zw', 'B.A.zw', 'z.B.A.w', 'A.Bz.w', 'B.w.Az', 'B.A.zw', 'A.B.zw', 'A.Bz.w', 'w.A.Bz', 'z.AB.w')
SPACE = 0.3
LAG = 4.0
DELAY = 2800
EAGER = 2
ORDER = ((0, -1), (1, -1), (2, -1), (3, -1), (4, -1), (5, -1), (6, -1), (7, -1), (8, -1), (9, -1), (10, -1), (11, -1), (12, -1), (13, -1), (14, -1), (15, -1), (0, 0), (1, 0), (2, 0), (3, 0), (4, 0), (5, 0), (6, 0), (7, 0), (8, 0), (9, 0), (10, 0), (11, 0), (12, 0), (13, 0), (14, 0), (15, 0), (0, 1), (1, 1), (2, 1), (3, 1), (4, 1), (5, 1), (6, 1), (7, 1), (8, 1), (9, 1), (10, 1), (11, 1), (12, 1), (13, 1), (14, 1), (15, 1), (1, 2), (2, 2), (3, 2), (4, 2), (5, 2), (8, 2), (9, 2), (10, 2), (14, 2), (15, 2), (1, 3), (4, 3), (11, 2), (7, 2), (0, 2), (5, 3), (6, 2), (12, 2), (13, 2), (3, 3), (2, 3), (8, 3))


def plane(wide):
    cores = 2 if wide % 2 == 0 else 1
    chips = wide // cores
    first = max(f for f in range(1, chips + 1) if chips % f == 0 and f * f <= chips)
    return first, chips // first, cores


def digits_of(axis, size):
    out, stride, f = [], 1, 2
    while stride < size:
        while (size // stride) % f:
            f += 1
        out.append((axis, f, stride))
        stride *= f
    return out


def radix(step):
    n = 1
    for d in step:
        n *= d[1]
    return n


def steps_of(pattern, dims):
    parts = {"A": dims[0], "B": dims[1], "z": dims[2][:1], "w": dims[2][1:]}
    steps = [tuple(d for c in step for d in parts[c]) for step in pattern.split(".")]
    return [step for step in steps if step]


def schedule(orders):
    ops = []
    if sorted(ORDER) == [(i, s) for i, steps in enumerate(orders) for s in range(-1, len(steps))]:
        return ORDER
    for i, steps in enumerate(orders):
        ops.append((i * SPACE, i, -1))
        for s in range(len(steps)):
            ops.append((i * SPACE + (s + 1) * LAG, i, s))
    return [(i, s) for _, i, s in sorted(ops)]


def kernel(
    sizes, orders, target, wl_index, tiles_in, mode_in, density_in, fwd, adj, shaped_out, norm_out,
    tile_of, mode, density, line, f_src, f_recv, w_src, w_recv, q_src, q_recv, slope, own, away, r0, recv, raw,
    in_sem, side_sem, pair_sem, swap_sem, step_sem, *bufs,
):
    g1, g2, cores, deep, groups, parts, rows, cols = sizes
    devices = g1 * g2 * cores * deep
    tile_rows = rows // devices
    per_core = g1 * g2 * deep
    width = cols // parts
    pieces = groups * parts
    f_bufs, a_bufs = bufs[:groups], bufs[groups:]
    w_me, z_me = lax.axis_index("wl"), lax.axis_index("tile")
    c_me = w_me % cores
    me = (w_me // (cores * g2), (w_me // cores) % g2, z_me, c_me)
    dims = [digits_of(0, g1), digits_of(1, g2), digits_of(2, deep), digits_of(3, cores)]

    def shift(coords, digit, o):
        axis, f, stride = digit
        d = (coords[axis] // stride) % f
        moved = coords[axis] + ((d + o) % f - d) * stride
        return coords[:axis] + (moved,) + coords[axis + 1 :]

    def split(digits, index):
        out = []
        for d in digits:
            out.append(index % d[1])
            index = index // d[1]
        return out

    def at(coords):
        a, b, z, c = coords
        return ((a * g2 + b) * cores + c, z)

    def flat(coords):
        w, z = at(coords)
        return w * deep + z

    def move(digits, index):
        coords = me
        for d, o in zip(digits, split(digits, index)):
            if not isinstance(o, int) or o:
                coords = shift(coords, d, o)
        return coords

    every = [d for axis in dims for d in axis]
    far = lambda j: -sum(d[2] * (d[0] != 3) + 0.5 for d, o in zip(every, split(every, j)) if o)
    others = sorted(range(1, devices), key=far)
    other = {j: at(move(every, j)) for j in others}

    barrier = pltpu.get_barrier_semaphore()
    for j in others:
        pl.semaphore_signal(barrier, inc=1, device_id=other[j], device_id_type=MESH)

    mon = rows // 2
    mt, mk, ms = mon // tile_rows, (mon % tile_rows) // SUB, mon % SUB
    line_copy = pltpu.make_async_copy(fwd.at[:, mt, mk], line, in_sem.at[2 * groups])
    mode_copy = pltpu.make_async_copy(mode_in, mode, side_sem.at[0])
    tile_copy = pltpu.make_async_copy(tiles_in, tile_of, side_sem.at[1])
    density_copy = pltpu.make_async_copy(density_in, density, side_sem.at[2])
    for copy in (line_copy, mode_copy, tile_copy):
        copy.start()
    loads = []
    for k in range(groups):
        pair = (
            pltpu.make_async_copy(fwd.at[:, :, k], f_bufs[k], in_sem.at[2 * k]),
            pltpu.make_async_copy(adj.at[:, :, k], a_bufs[k], in_sem.at[2 * k + 1]),
        )
        loads.append(pair)
    for pair in loads[:1]:
        for copy in pair:
            copy.start()

    line_copy.wait()
    mode_copy.wait()
    for pair in loads[1:]:
        for copy in pair:
            copy.start()
    density_copy.start()
    re, im = line[0, ms : ms + 1, :], line[1, ms : ms + 1, :]
    m_re, m_im = mode[0:1, :], mode[1:2, :]
    over_re = jnp.sum(re * m_re - im * m_im, axis=1, keepdims=True)
    over_im = jnp.sum(re * m_im + im * m_re, axis=1, keepdims=True)
    fom = jnp.broadcast_to((over_re * over_re + over_im * over_im) / cols, (1, LANES))
    f_src[...] = fom
    freq = 1.0 + wl_index[0].astype(jnp.float32) / devices
    aim, part = target[0] * (freq * freq), fom * (freq * freq)
    w_src[0:1, :] = jnp.full((1, LANES), aim)
    w_src[1:2, :] = part

    sem_of = {}
    for piece, steps in enumerate(orders):
        for s in range(len(steps)):
            sem_of[piece, s] = len(sem_of)
    flat_dims = dims[0] + dims[1] + dims[2]
    weights = []
    for steps in orders:
        weight, span = {}, per_core
        for step in steps:
            span //= radix(step)
            unit = span
            for d in step:
                weight[d] = unit
                unit *= d[1]
        weights.append(weight)
    kinds = sorted({tuple(w[d] for d in flat_dims) for w in weights})
    kind_of = [kinds.index(tuple(w[d] for d in flat_dims)) for w in weights]
    wide_dims = dims[0] + dims[1]

    tile_copy.wait()

    def build(k, some):
        for half in range(cores):

            @pl.loop(0, g1 * g2)
            def _(i):
                offs = split(wide_dims, i)
                coords = me
                for d, o in zip(wide_dims, offs):
                    coords = shift(coords, d, o)
                if half:
                    coords = shift(coords, dims[3][0], half)
                base = [sum(o * kind[n] for n, o in enumerate(offs)) for kind in kinds]
                for oz in range(deep):
                    zo = split(dims[2], oz)
                    there = coords
                    for d, o in zip(dims[2], zo):
                        if o:
                            there = shift(there, d, o)
                    t = tile_of[flat(there)]
                    for p in some:
                        cs = slice(p * width, (p + 1) * width)
                        piece = k * parts + p
                        kind = kind_of[piece]
                        slot = base[kind] + sum(o * kinds[kind][len(wide_dims) + n] for n, o in enumerate(zo))
                        (away if half else own)[piece, slot] = (
                            f_bufs[k][0, t, :, cs] * a_bufs[k][0, t, :, cs]
                            - f_bufs[k][1, t, :, cs] * a_bufs[k][1, t, :, cs]
                        )

    pl.semaphore_wait(barrier, devices - 1)

    def share(src, dst, sems):
        for j in others:
            pltpu.make_async_remote_copy(
                src_ref=src, dst_ref=dst.at[j - 1], send_sem=side_sem.at[sems], recv_sem=side_sem.at[sems + 1],
                device_id=other[j], device_id_type=MESH,
            ).start()
        return pltpu.make_async_remote_copy(
            src_ref=dst, dst_ref=dst, send_sem=side_sem.at[sems], recv_sem=side_sem.at[sems + 1],
            device_id=other[others[0]], device_id_type=MESH,
        )

    f_copy = share(f_src, f_recv, 3)
    partner = at(move(dims[3], 1)) if cores > 1 else None
    eager = range(min(EAGER, parts)) if cores == 2 and per_core > 1 else range(0)
    links = [(e, j, h) for e in eager for h in range(2) for j in range(1, radix(orders[e][0]))]

    def across(e, j, h):
        return at(move(list(orders[e][0]) + dims[3] * h, j + h * radix(orders[e][0])))

    def swap_of(src, dst, ssem, rsem):
        return pltpu.make_async_remote_copy(
            src_ref=src, dst_ref=dst, send_sem=ssem, recv_sem=rsem, device_id=partner, device_id_type=MESH
        )

    if cores > 1:
        for n, where in enumerate([partner] + [across(*link) for link in links]):
            pltpu.make_async_remote_copy(
                src_ref=w_src, dst_ref=w_recv.at[n], send_sem=pair_sem.at[0], recv_sem=pair_sem.at[1],
                device_id=where, device_id_type=MESH,
            ).start()
        w_copy = swap_of(w_recv, w_recv, pair_sem.at[0], pair_sem.at[1])

    def kept(piece):
        return per_core // radix(orders[piece][0]) if piece in eager else per_core

    def swap(piece):
        part = pl.ds(0, kept(piece))
        return swap_of(away.at[piece, part], r0.at[piece, part], pair_sem.at[2], swap_sem.at[piece])

    def swapped(k):
        part = pl.ds(k * parts, parts)
        return swap_of(away.at[part], r0.at[part], pair_sem.at[2], swap_sem.at[parts - 1 + k])

    def group_swap(piece):
        return swap_of(away.at[piece], r0.at[piece], pair_sem.at[2], swap_sem.at[parts - 1 + piece // parts])

    def swap_out(piece):
        (swap(piece) if piece < parts else group_swap(piece)).start()

    def send_raw(e):
        step, span = orders[e][0], kept(e)
        for h, src in enumerate((own, away)):
            for j in range(1, radix(step)):
                pltpu.make_async_remote_copy(
                    src_ref=src.at[e, pl.ds(j * span, span)],
                    dst_ref=raw.at[e, h, pl.ds((j - 1) * span, span)],
                    send_sem=pair_sem.at[2 + (h == 0)], recv_sem=step_sem.at[sem_of[e, 0]],
                    device_id=across(e, j, h), device_id_type=MESH,
                ).start()

    for k in range(groups):
        for copy in loads[k]:
            copy.wait()
        first = len(eager) if k == 0 else 0
        if first:
            build(k, range(first))
        for piece in range(k * parts, (k + 1) * parts):
            if piece in eager:
                send_raw(piece)
        if first < parts:
            build(k, range(first, parts))
        for piece in range(k * parts, (k + 1) * parts):
            if cores > 1:
                swap_out(piece)

    density_copy.wait()
    slope[...] = 4.0 * (1.0 - jnp.tanh(4.0 * (density[...] - 0.5)) ** 2)

    f_copy.wait_recv()
    total_fom = fom + jnp.sum(f_recv[...], axis=0)
    scale = total_fom / devices + 1.0

    def wide_factor(a, b):
        return jnp.broadcast_to(jnp.concatenate([a - b / scale] * (width // LANES), axis=1), (SUB, width))

    factor = wide_factor(aim, part)
    if cores > 1:
        w_copy.wait_recv()
        other_factor, *link_factors = [
            wide_factor(w_recv[n, 0:1, :], w_recv[n, 1:2, :]) for n in range(1 + len(links))
        ]
        link_factor = dict(zip(links, link_factors))

    spans, bases = [], []
    for steps in orders:
        span, base, ss, bs = per_core, 0, [], []
        for step in steps:
            span //= radix(step)
            ss.append(span)
            bs.append(base)
            base += (radix(step) - 1) * span
        spans.append(ss)
        bases.append(bs)

    def start(piece, s):
        step, span, base = orders[piece][s], spans[piece][s], bases[piece][s]
        for j in range(1, radix(step)):
            pltpu.make_async_remote_copy(
                src_ref=own.at[piece, pl.ds(j * span, span)],
                dst_ref=recv.at[piece, pl.ds(base + (j - 1) * span, span)],
                send_sem=pair_sem.at[3], recv_sem=step_sem.at[sem_of[piece, s]],
                device_id=at(move(step, j)), device_id_type=MESH,
            ).start()

    def take(piece, s):
        step, span, base = orders[piece][s], spans[piece][s], bases[piece][s]
        if s == 0 and piece in eager:
            got = raw.at[piece, :, pl.ds(0, (radix(step) - 1) * span)]
            pltpu.make_async_remote_copy(
                src_ref=got, dst_ref=got, send_sem=pair_sem.at[3], recv_sem=step_sem.at[sem_of[piece, 0]],
                device_id=at(move(step, 1)), device_id_type=MESH,
            ).wait_recv()
            value = own[piece, :span]
            for h in range(2):
                for j in range(1, radix(step)):
                    value = value + raw[piece, h, (j - 1) * span : j * span] * link_factor[piece, j, h]
            return value
        got = recv.at[piece, pl.ds(base, (radix(step) - 1) * span)]
        pltpu.make_async_remote_copy(
            src_ref=got, dst_ref=got, send_sem=pair_sem.at[3], recv_sem=step_sem.at[sem_of[piece, s]],
            device_id=at(move(step, 1)), device_id_type=MESH,
        ).wait_recv()
        value = own[piece, :span]
        for j in range(radix(step) - 1):
            value = value + recv[piece, base + j * span : base + (j + 1) * span]
        return value

    if DELAY:
        @pl.when(c_me == 1)
        def _():
            pl.delay(DELAY)

    squares = jnp.zeros((SUB, LANES), jnp.float32)
    opened = set()
    for piece, s in schedule(orders):
        steps = orders[piece]
        if s < 0:
            if cores > 1:
                if piece < parts:
                    swap(piece).wait_recv()
                elif piece // parts not in opened:
                    opened.add(piece // parts)
                    swapped(piece // parts).wait_recv()
                part = slice(0, kept(piece))
                own[piece, part] = own[piece, part] * factor + r0[piece, part] * other_factor
            else:
                own[piece] = own[piece] * factor
            if steps and piece not in eager:
                start(piece, 0)
        elif s < len(steps) - 1:
            own[piece, : spans[piece][s]] = take(piece, s)
            start(piece, s + 1)
        if s == len(steps) - 1:
            value = take(piece, s)[0] if steps else own[piece, 0]
            k, p = piece // parts, piece % parts
            rs, cs = slice(k * SUB, (k + 1) * SUB), slice(p * width, (p + 1) * width)
            shaped = value * slope[rs, cs]
            shaped_out[rs, cs] = shaped
            shaped = shaped * shaped
            for n in range(width // LANES):
                squares = squares + shaped[:, n * LANES : (n + 1) * LANES]
    mine = jnp.sum(squares, axis=0, keepdims=True)
    q_src[...] = mine
    q_copy = share(q_src, q_recv, 5)

    if cores > 1:
        w_copy.wait_send()
        swap_of(away, r0, pair_sem.at[2], pair_sem.at[2]).wait_send()
    if per_core > 1:
        sent = own.at[:, pl.ds(0, per_core - 1)]
        pltpu.make_async_remote_copy(
            src_ref=sent, dst_ref=sent, send_sem=pair_sem.at[3], recv_sem=pair_sem.at[3],
            device_id=other[others[0]], device_id_type=MESH,
        ).wait_send()
    f_copy.wait_send()
    q_copy.wait_recv()
    squares = jnp.sum(mine + jnp.sum(q_recv[...], axis=0), axis=1, keepdims=True)
    norm_out[...] = jnp.broadcast_to(jnp.sqrt(squares / (rows * cols) + 1e-06), (1, LANES))
    q_copy.wait_send()


def per_device(forward, adjoint, mode, target, wl_index, tile_of, density):
    wide, deep = lax.axis_size("wl"), lax.axis_size("tile")
    devices = wide * deep
    rows, cols = forward.shape[2:]
    g1, g2, cores = plane(wide)
    tile_rows = rows // devices
    groups = tile_rows // SUB
    parts = max(1, min(PIECES // groups, cols // LANES))
    pieces = groups * parts
    width = cols // parts
    per_core = g1 * g2 * deep
    dims = [digits_of(0, g1), digits_of(1, g2), digits_of(2, deep)]
    orders = [steps_of(PATTERNS[i % len(PATTERNS)], dims) for i in range(pieces)]
    eager = orders[: min(EAGER, parts)] if cores == 2 and per_core > 1 else []
    messages = 1 + sum(2 * (radix(steps[0]) - 1) for steps in eager)
    fwd = forward.reshape(2, devices, groups, SUB, cols)
    adj = adjoint.reshape(2, devices, groups, SUB, cols)
    f32 = jnp.float32
    dma = pltpu.SemaphoreType.DMA
    block = lambda n: pltpu.VMEM((pieces, n, SUB, width), f32)
    sizes = (g1, g2, cores, deep, groups, parts, rows, cols)
    peers = max(devices - 1, 1)
    vmem = pl.BlockSpec(memory_space=pltpu.VMEM)
    smem = pl.BlockSpec(memory_space=pltpu.SMEM)
    hbm = pl.BlockSpec(memory_space=pl.ANY)
    shaped, norm = pl.pallas_call(
        functools.partial(kernel, sizes, orders),
        out_shape=(pltpu.VMEM((tile_rows, cols), f32), pltpu.VMEM((1, LANES), f32)),
        in_specs=[smem, smem, hbm, hbm, hbm, hbm, hbm],
        out_specs=(vmem, vmem),
        scratch_shapes=[
            pltpu.SMEM((devices,), jnp.int32),
            pltpu.VMEM(mode.shape, f32),
            pltpu.VMEM((tile_rows, cols), f32),
            pltpu.VMEM((2, SUB, cols), f32),
            pltpu.VMEM((1, LANES), f32),
            pltpu.VMEM((peers, 1, LANES), f32),
            pltpu.VMEM((2, LANES), f32),
            pltpu.VMEM((messages, 2, LANES), f32),
            pltpu.VMEM((1, LANES), f32),
            pltpu.VMEM((peers, 1, LANES), f32),
            pltpu.VMEM((tile_rows, cols), f32),
            block(per_core),
            block(per_core),
            block(per_core),
            block(per_core),
            pltpu.VMEM((max(EAGER, 1), 2, per_core, SUB, width), f32),
            dma((2 * groups + 1,)),
            dma((7,)),
            dma((4,)),
            dma((parts + groups - 1,)),
            dma((max(sum(len(steps) for steps in orders), 1),)),
        ]
        + [pltpu.VMEM((2, devices, SUB, cols), f32)] * (2 * groups),
        compiler_params=pltpu.CompilerParams(
            collective_id=0, has_side_effects=True, vmem_limit_bytes=60 * 2**20
        ),
        name="assemble",
    )(target, wl_index, tile_of, mode, density, fwd, adj)
    return shaped / norm[0, 0]


def solution(mesh):
    in_specs = (
        P(("wl", "tile"), None, None, None),
        P(("wl", "tile"), None, None, None),
        P(),
        P(("wl", "tile")),
        P(("wl", "tile")),
        P(),
        P(("wl", "tile"), None),
    )
    out_specs = P(("wl", "tile"), None)
    return jax.shard_map(
        per_device, mesh=mesh, in_specs=in_specs, out_specs=out_specs, check_vma=False
    )
```
